256 devices in a mesh: parts: 4 (over y, x), dp: 64 (over z, core).
Axes of the slice: x: 2, y: 2, z: 32, core: 2. Of those that a mesh axis runs over, the one named last changes fastest.
The devices are a block of a 4x8x32 slice.
Arguments:
- activations: bfloat16 [65536, 14336], P(('parts', 'dp')), parts along dimension 0, may hold values from -6 to 6
- out_grads: bfloat16 [65536, 4096], P(('parts', 'dp')), parts along dimension 0, may hold values from -6 to 6
- lengths: int32 [256, 4], P(('parts', 'dp')), parts along dimension 0, may hold values from 1 to 128, 256 in all within a row
- proj_in: bfloat16 [14336, 64], replicated, may hold values from -0.046875 to 0.046875
- proj_out: bfloat16 [4096, 64], replicated, may hold values from -0.09375 to 0.09375
- queries: bfloat16 [8192, 4096], P(('parts', 'dp')), parts along dimension 0, may hold values from -0.01171875 to 0.01171875
Outputs:
- scores: bfloat16 [1024, 2048], P(('parts', 'dp')), parts along dimension 0
The draws below stay inside these ranges and needn't reach their ends.
There are 4 independent parts, one for each index of `parts`. The reference program is written for one: setup_inputs(seed, part) draws one part's arguments, and reference() takes and returns one part's arrays. A program takes and returns all parts, laid end to end along the dimension named above; an argument that names none is the same for every part. Nothing has to cross between parts.
Inputs may be any that keep to these rules, and one draw needn't show every extreme that they name: Each row of lengths sums to 256, and one entry of each row equals 128.
All inputs are finite; a program needn't handle non-finite values.
Results may differ from the reference program's by a relative error of at most 0.0065.
Values may be sent and summed in bfloat16 or wider, within the bound.
A program may use at most 128 MiB of HBM per device.

```python
import math
import jax
import jax.numpy as jnp
import numpy as np

D = 4096
FF = 14336
RANK = 64
TOK_DEV = 256
EX_DEV = 4
TOKENS = 16384
N_TRAIN = 256
NQ = 2048
PARAMS = 4096
MOST = 128
N_DP = 64


def level_of(rng, dims, pieces, smallest, top_value):
    level = 1.0
    for dim, shards_of in pieces:
        heights = jax.random.uniform(jax.random.fold_in(jax.random.fold_in(rng, 6), dim), (shards_of,), jnp.float32, smallest / len(pieces), top_value / len(pieces))
        level = level * jnp.repeat(jnp.exp(heights), dims[dim] // shards_of).reshape((-1,) + (1,) * (len(dims) - 1 - dim))
    return level


def split_up(number_of, total, reach, lean):
    weights = [(1 << 20) // math.isqrt(standing ** lean) + 1 for standing in range(2, number_of + 1)]
    surplus, holding = total - reach - (number_of - 1), [1] * (number_of - 1)
    while surplus > 0:
        free = [i for i in range(number_of - 1) if holding[i] < reach]
        mass, remaining = sum([weights[i] for i in free]), surplus
        for i in free:
            more = min(reach - holding[i], max(1, remaining * weights[i] // mass), surplus)
            holding[i] = holding[i] + more
            surplus = surplus - more
    return np.array([reach] + holding)


def uneven(own_key, count, total, reach, lean):
    if count == 2:
        one = jax.random.randint(own_key, (), max(1, total - reach), min(reach, total - 1) + 1)
        return jnp.stack([one, total - one])
    sizes = jnp.asarray(split_up(count, total, reach, lean), jnp.int32)
    twos = (count - 1) // 2
    giver, sink = sizes[1:1 + 2 * twos:2], sizes[2:2 + 2 * twos:2]
    room = jnp.minimum(giver - 1, reach - sink)
    shifted = jax.random.randint(jax.random.fold_in(own_key, 1), (twos,), 0, 1 << 20) % (room + 1)
    sizes = sizes.at[1:1 + 2 * twos:2].set(giver - shifted).at[2:2 + 2 * twos:2].set(sink + shifted)
    return sizes[jax.random.permutation(jax.random.fold_in(own_key, 2), count)]


def scatter_about(own_key, extent, spread, reach, pieces=(), kind=jnp.bfloat16):
    entries = spread * jax.random.normal(own_key, extent, jnp.float32)
    if pieces:
        entries = entries * level_of(own_key, extent, pieces, -0.22, 0.18)
    return jnp.clip(entries, -reach, reach).astype(kind)


def setup_inputs(seed: int = 0, part: int = 0) -> dict:
    key_of = jax.random.split(jax.random.key(seed), 7)
    part_keys = jax.random.split(jax.random.fold_in(key_of[6], part), 7)
    activations = scatter_about(part_keys[0], (TOKENS, FF), 1.0, 6.0, ((0, 64),))
    out_grads = scatter_about(part_keys[1], (TOKENS, D), 1.0, 6.0, ((0, 64),))
    lengths = jax.vmap(lambda own: uneven(own, EX_DEV, TOK_DEV, MOST, 2))(jax.random.split(part_keys[2], N_DP)).reshape((N_DP, EX_DEV)).astype(jnp.int32)
    proj_in = scatter_about(key_of[3], (FF, RANK), FF ** -0.5, 0.046875)
    proj_out = scatter_about(key_of[4], (D, RANK), D ** -0.5, 0.09375)
    queries = scatter_about(part_keys[5], (NQ, PARAMS), (0.125 / RANK), 0.01171875, ((0, 64),))
    return dict(activations=activations, out_grads=out_grads, lengths=lengths, proj_in=proj_in, proj_out=proj_out, queries=queries)


def reference(activations, out_grads, lengths, proj_in, proj_out, queries):
    proj_acts = jnp.dot(activations, proj_in, preferred_element_type=jnp.float32).astype(jnp.bfloat16)
    proj_grads = jnp.dot(out_grads, proj_out, preferred_element_type=jnp.float32).astype(jnp.bfloat16)
    acts_wide = proj_acts.astype(jnp.float32)
    grads_wide = proj_grads.astype(jnp.float32)
    outer_terms = (grads_wide[:, :, None] * acts_wide[:, None, :]).reshape(TOKENS, RANK * RANK)
    tok_ends = jnp.cumsum(lengths.reshape(-1)).astype(jnp.int32)
    position = jnp.arange(TOKENS, dtype=jnp.int32)
    example_ids = jnp.searchsorted(tok_ends, position, side="right").astype(jnp.int32)
    example_grads = jax.ops.segment_sum(outer_terms, example_ids, num_segments=N_TRAIN).astype(jnp.bfloat16)
    return jnp.dot(example_grads, queries.T, preferred_element_type=jnp.float32).astype(jnp.bfloat16)
```

```python
import jax
import jax.numpy as jnp
from jax import lax
from jax.sharding import PartitionSpec as P


def local(activations, out_grads, lengths, proj_in, proj_out, queries):
    tok_count = activations.shape[0]
    rank_size = proj_in.shape[1]
    proj_acts = jnp.dot(activations, proj_in, preferred_element_type=jnp.float32).astype(
        jnp.bfloat16
    )
    proj_grads = jnp.dot(out_grads, proj_out, preferred_element_type=jnp.float32).astype(
        jnp.bfloat16
    )
    counts = lengths[0]
    examples = counts.shape[0]
    position = jnp.arange(tok_count, dtype=jnp.int32)
    tok_ends = [counts[0]]
    for e in range(1, examples):
        tok_ends.append(tok_ends[-1] + counts[e])
    owner = sum((position >= end).astype(jnp.int32) for end in tok_ends[:-1])
    member = (owner[:, None] == jnp.arange(examples)[None, :]).astype(jnp.bfloat16)
    masked = (member[:, :, None] * proj_acts[:, None, :]).reshape(tok_count, examples * rank_size)
    summed = lax.dot_general(
        proj_grads, masked, (((0,), (0,)), ((), ())), preferred_element_type=jnp.float32
    )
    example_grads = (
        summed.reshape(rank_size, examples, rank_size)
        .transpose(1, 0, 2)
        .reshape(examples, rank_size * rank_size)
        .astype(jnp.bfloat16)
    )
    contract = (((1,), (1,)), ((), ()))
    scores = lax.dot_general(
        lax.all_gather(example_grads, "dp", axis=0, tiled=True),
        queries,
        contract,
        preferred_element_type=jnp.float32,
    ).astype(jnp.bfloat16)
    return lax.all_to_all(scores, "dp", split_axis=0, concat_axis=1, tiled=True)


def solution(mesh):
    in_specs = (
        P(("parts", "dp"), None),
        P(("parts", "dp"), None),
        P(("parts", "dp"), None),
        P(),
        P(),
        P(("parts", "dp"), None),
    )
    out_specs = P(("parts", "dp"), None)
    return jax.shard_map(local, mesh=mesh, in_specs=in_specs, out_specs=out_specs, check_vma=False)
```

```python
import functools

import jax
import jax.numpy as jnp
from jax import lax
from jax.experimental import pallas as pl
from jax.experimental.pallas import tpu as pltpu
from jax.sharding import PartitionSpec as P

MESH = pl.DeviceIdType.MESH
STRIDE = 4
F32 = jnp.float32
BF16 = jnp.bfloat16
NT = (((1,), (1,)), ((), ()))


def cuts(total, size):
    widths = [size] * (total // size)
    if total % size:
        widths.append(total % size)
    if widths[-1] % 256 == 0 and widths[-1] >= 512:
        widths[-1:] = [widths[-1] // 2] * 2
    starts = [sum(widths[:i]) for i in range(len(widths))]
    return list(zip(starts, widths))


def kernel(
    nz, chunk, acts, grads, lens, pin, pout, qs, out,
    abuf, gbuf, pinb, poutb, qv, qbuf, ybuf, rbuf, sbuf, res,
    loc_sem, qloc_sem, qsend, qrecv, dsend, fsend, erecv, rsend, rrecv,
):
    me = lax.axis_index("dp")
    z, core = me // 2, lax.rem(me, 2)
    part = lax.rem(z, STRIDE)
    groups = nz // (2 * STRIDE)
    blocks = 2 * STRIDE
    toks, ff = acts.shape
    d = grads.shape[1]
    rank = pin.shape[0]
    kq = qs.shape[1] // STRIDE

    def chip(dz):
        return lax.rem(z + nz + dz, nz)

    def dev(dz):
        return {"dp": chip(dz) * 2 + core}

    partner = {"dp": z * 2 + 1 - core}

    def remote(src, dst, ssem, rsem, to):
        return pltpu.make_async_remote_copy(
            src_ref=src, dst_ref=dst, send_sem=ssem, recv_sem=rsem,
            device_id=to, device_id_type=MESH,
        )

    barrier = pltpu.get_barrier_semaphore()
    near = [dz for t in range(1, STRIDE + 1) for dz in (t, -t)]
    for dz in near:
        pl.semaphore_signal(barrier, inc=1, device_id=dev(dz), device_id_type=MESH)
    pl.semaphore_signal(barrier, inc=1, device_id=partner, device_id_type=MESH)

    def q_cols(dz):
        return pl.ds(pl.multiple_of(lax.rem(z + nz + dz, STRIDE) * kq, kq), kq)

    q_all = pltpu.make_async_copy(qs, qv, qloc_sem.at[0])
    q_own = pltpu.make_async_copy(qs.at[:, q_cols(0)], qbuf.at[part * 2 + core], qloc_sem.at[1])
    q_all.start()
    q_own.start()
    n_sem = 0
    g_chunks, a_chunks = [], []
    pout_copy = pltpu.make_async_copy(pout, poutb, loc_sem.at[n_sem])
    pout_copy.start()
    n_sem += 1
    for lo, w in cuts(d, chunk):
        cp = pltpu.make_async_copy(
            grads.at[:, pl.ds(lo, w)], gbuf.at[:, pl.ds(lo, w)], loc_sem.at[n_sem]
        )
        cp.start()
        n_sem += 1
        g_chunks.append((lo, w, cp))
    for lo, w in cuts(ff, chunk):
        cp0 = pltpu.make_async_copy(
            pin.at[:, pl.ds(lo, w)], pinb.at[:, pl.ds(lo, w)], loc_sem.at[n_sem]
        )
        cp1 = pltpu.make_async_copy(
            acts.at[:, pl.ds(lo, w)], abuf.at[:, pl.ds(lo, w)], loc_sem.at[n_sem + 1]
        )
        cp0.start()
        cp1.start()
        n_sem += 2
        a_chunks.append((lo, w, cp0, cp1))

    pg = jnp.zeros((toks, rank), F32)
    pout_copy.wait()
    for lo, w, cp in g_chunks:
        cp.wait()
        pg = pg + lax.dot_general(
            gbuf[:, lo : lo + w], poutb[:, lo : lo + w], NT, preferred_element_type=F32
        )
    pg = pg.astype(BF16)
    rows = 4 * rank
    r = lax.broadcasted_iota(jnp.int32, (rows, rank), 0)
    i = lax.broadcasted_iota(jnp.int32, (rows, rank), 1)
    quarter = r // rank
    i_lo = (quarter & 1) * 2 + quarter // 2
    spread = (i == ((r & (rank - 1)) & ~3) + i_lo).astype(F32).astype(BF16)
    wide = lax.dot_general(spread, pg, NT, preferred_element_type=F32)
    e = lax.broadcasted_iota(jnp.int32, (rows, toks), 0) & 3
    tok = lax.broadcasted_iota(jnp.int32, (rows, toks), 1)
    end0 = lens[0, 0]
    end1 = end0 + lens[0, 1]
    end2 = end1 + lens[0, 2]
    owner = (
        (tok >= end0).astype(jnp.int32)
        + (tok >= end1).astype(jnp.int32)
        + (tok >= end2).astype(jnp.int32)
    )
    lhs = jnp.where(owner == e, wide, 0.0).astype(BF16)

    pa = jnp.zeros((toks, 2 * rank), F32)
    q_sends = []
    for n, (lo, w, cp0, cp1) in enumerate(a_chunks):
        if n == len(a_chunks) // 2:
            q_all.wait()
            pl.semaphore_wait(barrier, len(near) + 1)
            slot = part * 2 + core
            for k, dz in enumerate((1, -1)):
                q_sends.append(
                    remote(qv.at[:, q_cols(dz)], qbuf.at[slot], qsend.at[k], qrecv.at[k], dev(dz))
                )
            far = {"dp": lax.rem(z + nz + 2 - 4 * core, nz) * 2 + core}
            q_sends.append(
                remote(qv.at[:, q_cols(2)], qbuf.at[slot], qsend.at[2], qrecv.at[2], far)
            )
            q_sends.append(
                remote(qv.at[:, q_cols(0)], qbuf.at[slot], qsend.at[3], qrecv.at[3], partner)
            )
            for cp in q_sends:
                cp.start()
        cp0.wait()
        cp1.wait()
        p = pinb[:, lo : lo + w]
        pa = pa + lax.dot_general(
            abuf[:, lo : lo + w], jnp.concatenate([p, p], axis=0), NT, preferred_element_type=F32
        )
    left = lax.broadcasted_iota(jnp.int32, (toks, 2 * rank), 1) < rank
    pa_l = jnp.where(left, pa, 0.0).astype(BF16)
    pa_r = jnp.where(left, 0.0, pa).astype(BF16)
    half = 2 * rank
    y = jnp.dot(lhs[:half], pa_l, preferred_element_type=F32) + jnp.dot(
        lhs[half:], pa_r, preferred_element_type=F32
    )
    y = jnp.concatenate([y[:rank], y[rank:]], axis=1).astype(BF16)
    own_rows = rank // STRIDE
    for s in range(STRIDE):
        ybuf[s] = y[s * own_rows : (s + 1) * own_rows]

    def slot_of(m, direction, t):
        return m * blocks + direction * STRIDE + t - 1

    last = groups * blocks - 1
    direct = []
    for t in range(STRIDE, 0, -1):
        for direction in (0, 1):
            k = slot_of(0, direction, t)
            if k == last:
                continue
            dz = t if direction == 0 else -t
            direct.append(
                remote(
                    ybuf.at[lax.rem(z + nz + dz, STRIDE)], rbuf.at[k],
                    dsend.at[k], erecv.at[k], dev(dz),
                )
            )
            direct[-1].start()
    rbuf[last] = ybuf[part]

    q_own.wait()
    passed = []
    for k in range(3):
        if k == 0:
            from_slot = lax.rem(z + nz - 1, STRIDE) * 2 + core
        elif k == 1:
            from_slot = lax.rem(z + 1, STRIDE) * 2 + core
        else:
            from_slot = lax.rem(z + 2, STRIDE) * 2 + core
        q_sends[k].wait_recv()
        passed.append(
            remote(
                qbuf.at[from_slot], qbuf.at[from_slot], qsend.at[4 + k], qrecv.at[4 + k], partner
            )
        )
        passed[-1].start()

    def arrival(k):
        return remote(rbuf.at[k], rbuf.at[k], fsend.at[k], erecv.at[k], dev(STRIDE))

    forwards, returns = [], []
    sub = lax.broadcasted_iota(jnp.int32, (blocks, 8, 128), 1) < 4
    for m in range(groups):
        for t in range(STRIDE, 0, -1):
            for direction in (0, 1):
                k = slot_of(m, direction, t)
                if k == last:
                    continue
                arrival(k).wait_recv()
                nxt = k + blocks
                if nxt < groups * blocks and nxt != last:
                    fw = remote(
                        rbuf.at[k], rbuf.at[nxt], fsend.at[k], erecv.at[nxt],
                        dev(STRIDE if direction == 0 else -STRIDE),
                    )
                    fw.start()
                    forwards.append(fw)
        if m == 0:
            q_sends[3].wait_recv()
            for cp in passed:
                cp.wait_recv()
        held = rbuf[m * blocks : (m + 1) * blocks].reshape(blocks * own_rows, 4 * rank)
        prods = []
        for g in range(STRIDE):
            w = qbuf[:, :, g * 256 : (g + 1) * 256].reshape(-1, 256)
            pr = lax.dot_general(held, w, NT, preferred_element_type=F32)
            pr = pr.reshape(blocks, own_rows, pr.shape[-1])
            prods.append(pr[:, 8 * (g // 2) : 8 * (g // 2) + 8])
        packed = []
        for h in range(2):
            c0, c1 = h * 128, (h + 1) * 128
            s = jnp.where(sub, prods[0][:, :, c0:c1], prods[1][:, :, c0:c1])
            s = s + jnp.where(sub, prods[2][:, :, c0:c1], prods[3][:, :, c0:c1])
            packed.append(s + pltpu.roll(s, 4, 1))
        sbuf[m * blocks : (m + 1) * blocks] = jnp.where(sub, packed[0], packed[1]).astype(BF16)
        for t in range(STRIDE, 0, -1):
            for direction in (0, 1):
                k = slot_of(m, direction, t)
                if k == last:
                    continue
                dist = m * STRIDE + t
                back = remote(
                    sbuf.at[k], res.at[z], rsend.at[k], rrecv.at[z],
                    dev(-dist if direction == 0 else dist),
                )
                back.start()
                returns.append(back)
    res[z] = sbuf[last]

    for dz in range(1, nz):
        src = chip(dz)
        remote(res.at[src], res.at[src], rsend.at[0], rrecv.at[src], partner).wait_recv()

    row = lax.broadcasted_iota(jnp.int32, (8, 128), 0)
    lane = lax.broadcasted_iota(jnp.int32, (8, 128), 1)
    col = (row // 4) * 128 + lane
    segments = nz // STRIDE
    acc = [jnp.zeros((8, 128), F32) for _ in range(segments)]
    for rho in range(STRIDE):
        gap = (col // 64 - rho + STRIDE) & (STRIDE - 1)
        shift = jnp.where(gap == 3, -1, gap)
        shift = jnp.where(gap == 2, jnp.where((col // 32) % 2 == 0, -2, 2), shift)
        target = rho + shift
        seg_masks = {-1: target < 0, 0: (target >= 0) & (target < STRIDE), 1: target >= STRIDE}
        used = {0} | ({-1} if rho < 2 else set()) | ({1} if rho >= STRIDE - 2 else set())
        for s in range(segments):
            val = res[s * STRIDE + rho].astype(F32)
            for rel in sorted(used):
                to = (s + rel) % segments
                acc[to] = acc[to] + jnp.where(seg_masks[rel], val, 0.0)
    for s in range(segments):
        out[:, s * 256 : s * 256 + 128] = acc[s][:4].astype(out.dtype)
        out[:, s * 256 + 128 : s * 256 + 256] = acc[s][4:].astype(out.dtype)

    for cp in q_sends + passed + direct + forwards + returns:
        cp.wait_send()


def local(nz, activations, out_grads, lengths, proj_in, proj_out, queries):
    toks, ff = activations.shape
    d = out_grads.shape[1]
    rank = proj_in.shape[1]
    nq, params = queries.shape
    chunk = min(2048, d)
    n_loc = 1 + len(cuts(d, chunk)) + 2 * len(cuts(ff, chunk))
    dma = pltpu.SemaphoreType.DMA
    anyspec = pl.BlockSpec(memory_space=pl.ANY)
    rows = rank // STRIDE
    return pl.pallas_call(
        functools.partial(kernel, nz, chunk),
        out_shape=jax.ShapeDtypeStruct((lengths.shape[1], 2 * nz * nq), BF16),
        in_specs=[
            anyspec, anyspec, pl.BlockSpec(memory_space=pltpu.SMEM), anyspec, anyspec, anyspec,
        ],
        out_specs=pl.BlockSpec(memory_space=pltpu.VMEM),
        scratch_shapes=[
            pltpu.VMEM((toks, ff), BF16),
            pltpu.VMEM((toks, d), BF16),
            pltpu.VMEM((rank, ff), BF16),
            pltpu.VMEM((rank, d), BF16),
            pltpu.VMEM((nq, params), BF16),
            pltpu.VMEM((2 * STRIDE, nq, params // STRIDE), BF16),
            pltpu.VMEM((STRIDE, rows, 4 * rank), BF16),
            pltpu.VMEM((nz, rows, 4 * rank), BF16),
            pltpu.VMEM((nz, 8, 128), BF16),
            pltpu.VMEM((nz, 8, 128), BF16),
            dma((n_loc,)), dma((2,)), dma((7,)), dma((7,)), dma((2 * STRIDE,)),
            dma((nz,)), dma((nz,)), dma((nz,)), dma((nz,)),
        ],
        compiler_params=pltpu.CompilerParams(collective_id=0, has_side_effects=True),
        name="score",
    )(activations, out_grads, lengths, proj_in.T, proj_out.T, queries)


def solution(mesh):
    both = P(("parts", "dp"), None)
    in_specs = (both, both, both, P(), P(), both)
    body = functools.partial(local, mesh.shape["dp"] // 2)
    return jax.shard_map(body, mesh=mesh, in_specs=in_specs, out_specs=both, check_vma=False)
```

```python
import functools

import jax
import jax.numpy as jnp
from jax import lax
from jax.experimental import pallas as pl
from jax.experimental.pallas import tpu as pltpu
from jax.sharding import PartitionSpec as P

MESH = pl.DeviceIdType.MESH
STRIDE = 4
F32 = jnp.float32
BF16 = jnp.bfloat16
NT = (((1,), (1,)), ((), ()))


def cuts(total, size):
    widths = [size] * (total // size)
    if total % size:
        widths.append(total % size)
    if widths[-1] % 256 == 0 and widths[-1] >= 512:
        widths[-1:] = [widths[-1] // 2] * 2
    starts = [sum(widths[:i]) for i in range(len(widths))]
    return list(zip(starts, widths))


def split(nz):
    total = nz // STRIDE
    up = max(total * 5 // 8, total // 2)
    return up, total - up


def kernel(
    nz, chunk, acts, grads, lens, pin, pout, qs, out,
    abuf, gbuf, pinb, poutb, qv, qbuf, ybuf, rbuf, sbuf, res,
    loc_sem, qloc_sem, qsend, qrecv, dsend, fsend, erecv, rsend, rrecv, wrap_sem,
):
    me = lax.axis_index("dp")
    z, core = me // 2, lax.rem(me, 2)
    part = lax.rem(z, STRIDE)
    r_groups, l_groups = split(nz)
    blocks = 2 * STRIDE
    toks, ff = acts.shape
    d = grads.shape[1]
    rank = pin.shape[0]
    kq = qs.shape[1] // STRIDE

    def chip(dz):
        return lax.rem(z + nz + dz, nz)

    def dev(dz):
        return {"dp": chip(dz) * 2 + core}

    partner = {"dp": z * 2 + 1 - core}

    def remote(src, dst, ssem, rsem, to):
        return pltpu.make_async_remote_copy(
            src_ref=src, dst_ref=dst, send_sem=ssem, recv_sem=rsem,
            device_id=to, device_id_type=MESH,
        )

    barrier = pltpu.get_barrier_semaphore()
    near = [dz for t in range(1, STRIDE + 1) for dz in (t, -t)]

    def greet(sem, dz):
        pl.semaphore_signal(sem, inc=1, device_id=dev(dz), device_id_type=MESH)

    for dz in near:
        if dz < 0:
            greet(barrier, dz)
        else:
            pl.when(z + dz < nz)(functools.partial(greet, barrier, dz))
    pl.semaphore_signal(barrier, inc=1, device_id=partner, device_id_type=MESH)

    def await_near():
        pl.semaphore_wait(barrier, len(near) + 1 - jnp.maximum(STRIDE - z, 0))
        for dz in range(1, STRIDE + 1):
            pl.when(z + dz >= nz)(functools.partial(greet, wrap_sem, dz))

    def q_cols(dz):
        return pl.ds(pl.multiple_of(lax.rem(z + nz + dz, STRIDE) * kq, kq), kq)

    q_all = pltpu.make_async_copy(qs, qv, qloc_sem.at[0])
    q_own = pltpu.make_async_copy(qs.at[:, q_cols(0)], qbuf.at[part * 2 + core], qloc_sem.at[1])
    q_all.start()
    q_own.start()
    n_sem = 0
    g_chunks, a_chunks = [], []
    pout_copy = pltpu.make_async_copy(pout, poutb, loc_sem.at[n_sem])
    pout_copy.start()
    n_sem += 1
    for lo, w in cuts(d, chunk):
        cp = pltpu.make_async_copy(
            grads.at[:, pl.ds(lo, w)], gbuf.at[:, pl.ds(lo, w)], loc_sem.at[n_sem]
        )
        cp.start()
        n_sem += 1
        g_chunks.append((lo, w, cp))
    for lo, w in cuts(ff, chunk):
        cp0 = pltpu.make_async_copy(
            pin.at[:, pl.ds(lo, w)], pinb.at[:, pl.ds(lo, w)], loc_sem.at[n_sem]
        )
        cp1 = pltpu.make_async_copy(
            acts.at[:, pl.ds(lo, w)], abuf.at[:, pl.ds(lo, w)], loc_sem.at[n_sem + 1]
        )
        cp0.start()
        cp1.start()
        n_sem += 2
        a_chunks.append((lo, w, cp0, cp1))

    pg = jnp.zeros((toks, rank), F32)
    pout_copy.wait()
    for lo, w, cp in g_chunks:
        cp.wait()
        pg = pg + lax.dot_general(
            gbuf[:, lo : lo + w], poutb[:, lo : lo + w], NT, preferred_element_type=F32
        )
    pg = pg.astype(BF16)
    rows = 4 * rank
    r = lax.broadcasted_iota(jnp.int32, (rows, rank), 0)
    i = lax.broadcasted_iota(jnp.int32, (rows, rank), 1)
    quarter = r // rank
    i_lo = (quarter & 1) * 2 + quarter // 2
    spread = (i == ((r & (rank - 1)) & ~3) + i_lo).astype(F32).astype(BF16)
    wide = lax.dot_general(spread, pg, NT, preferred_element_type=F32)
    e = lax.broadcasted_iota(jnp.int32, (rows, toks), 0) & 3
    tok = lax.broadcasted_iota(jnp.int32, (rows, toks), 1)
    end0 = lens[0, 0]
    end1 = end0 + lens[0, 1]
    end2 = end1 + lens[0, 2]
    owner = (
        (tok >= end0).astype(jnp.int32)
        + (tok >= end1).astype(jnp.int32)
        + (tok >= end2).astype(jnp.int32)
    )
    lhs = jnp.where(owner == e, wide, 0.0).astype(BF16)

    pa = jnp.zeros((toks, 2 * rank), F32)
    slot = part * 2 + core
    q_up = remote(qv.at[:, q_cols(1)], qbuf.at[slot], qsend.at[0], qrecv.at[0], dev(1))
    q_down = remote(qv.at[:, q_cols(-1)], qbuf.at[slot], qsend.at[1], qrecv.at[1], dev(-1))
    far = {"dp": lax.rem(z + nz + 2 - 4 * core, nz) * 2 + core}
    q_far = remote(qv.at[:, q_cols(2)], qbuf.at[slot], qsend.at[2], qrecv.at[2], far)
    q_near = remote(qv.at[:, q_cols(0)], qbuf.at[slot], qsend.at[3], qrecv.at[3], partner)
    q_sends = [q_up, q_down, q_far, q_near]
    for n, (lo, w, cp0, cp1) in enumerate(a_chunks):
        if n == len(a_chunks) // 2:
            q_all.wait()
            await_near()
            q_up.start()
            q_near.start()
            pl.when((z >= STRIDE) | (core == 0))(q_far.start)
            pl.when(z >= STRIDE)(q_down.start)
        cp0.wait()
        cp1.wait()
        p = pinb[:, lo : lo + w]
        pa = pa + lax.dot_general(
            abuf[:, lo : lo + w], jnp.concatenate([p, p], axis=0), NT, preferred_element_type=F32
        )
    left = lax.broadcasted_iota(jnp.int32, (toks, 2 * rank), 1) < rank
    pa_l = jnp.where(left, pa, 0.0).astype(BF16)
    pa_r = jnp.where(left, 0.0, pa).astype(BF16)
    half = 2 * rank
    y = jnp.dot(lhs[:half], pa_l, preferred_element_type=F32) + jnp.dot(
        lhs[half:], pa_r, preferred_element_type=F32
    )
    y = jnp.concatenate([y[:rank], y[rank:]], axis=1).astype(BF16)
    own_rows = rank // STRIDE
    for s in range(STRIDE):
        ybuf[s] = y[s * own_rows : (s + 1) * own_rows]

    def base(m):
        return m * blocks if m < l_groups else l_groups * blocks + (m - l_groups) * STRIDE

    def slot_of(m, up, t):
        return base(m) + (0 if up else STRIDE) + t - 1

    last = slot_of(l_groups - 1, False, STRIDE)

    def leg(up, t):
        k = slot_of(0, up, t)
        dz = t if up else -t
        return remote(
            ybuf.at[lax.rem(z + nz + dz, STRIDE)], rbuf.at[k], dsend.at[k], erecv.at[k], dev(dz)
        )

    hops = range(STRIDE, 0, -1)
    ups = [leg(True, t) for t in hops]
    downs = [leg(False, t) for t in hops if slot_of(0, False, t) != last]
    for cp in ups:
        cp.start()

    def start_downs():
        for cp in downs:
            cp.start()

    def after_wrap():
        pl.semaphore_wait(wrap_sem, STRIDE - z)
        q_down.start()
        pl.when(core == 1)(q_far.start)
        start_downs()

    pl.when(z >= STRIDE)(start_downs)
    rbuf[last] = ybuf[part]
    q_own.wait()

    forwards, returns, passed = [], [], []

    def pass_on(k, up, nxt):
        remote(rbuf.at[k], rbuf.at[k], fsend.at[k], erecv.at[k], dev(STRIDE)).wait_recv()
        if nxt is not None and nxt != last:
            fw = remote(
                rbuf.at[k], rbuf.at[nxt], fsend.at[k], erecv.at[nxt], dev(STRIDE if up else -STRIDE)
            )
            fw.start()
            forwards.append(fw)

    def returning(k, dist):
        back = remote(sbuf.at[k], res.at[z], rsend.at[k], rrecv.at[z], dev(dist))
        back.start()
        returns.append(back)

    for m in range(r_groups):
        for t in range(1, STRIDE + 1):
            if m == 0:
                pl.when(z == t - 1)(after_wrap)
            pass_on(
                slot_of(m, True, t), True, slot_of(m + 1, True, t) if m + 1 < r_groups else None
            )
        if m == 0:
            for k, dz in enumerate((-1, 1, 2)):
                came = lax.rem(z + nz + dz, STRIDE) * 2 + core
                q_sends[k].wait_recv()
                passed.append(
                    remote(
                        qbuf.at[came], qbuf.at[came], qsend.at[4 + k], qrecv.at[4 + k], partner
                    )
                )
                passed[-1].start()
        if m < l_groups:
            for t in range(1, STRIDE + 1):
                if slot_of(m, False, t) != last:
                    pass_on(
                        slot_of(m, False, t), False,
                        slot_of(m + 1, False, t) if m + 1 < l_groups else None,
                    )
        if m == 0:
            q_near.wait_recv()
            for cp in passed:
                cp.wait_recv()
        count = blocks if m < l_groups else STRIDE
        held = rbuf[base(m) : base(m) + count].reshape(count * own_rows, 4 * rank)
        prods = []
        for g in range(STRIDE):
            w = qbuf[:, :, g * 256 : (g + 1) * 256].reshape(-1, 256)
            pr = lax.dot_general(held, w, NT, preferred_element_type=F32)
            pr = pr.reshape(count, own_rows, pr.shape[-1])
            prods.append(pr[:, 8 * (g // 2) : 8 * (g // 2) + 8])
        sub = lax.broadcasted_iota(jnp.int32, (count, 8, 128), 1) < 4
        packed = []
        for h in range(2):
            c0, c1 = h * 128, (h + 1) * 128
            s = jnp.where(sub, prods[0][:, :, c0:c1], prods[1][:, :, c0:c1])
            s = s + jnp.where(sub, prods[2][:, :, c0:c1], prods[3][:, :, c0:c1])
            packed.append(s + pltpu.roll(s, 4, 1))
        sbuf[base(m) : base(m) + count] = jnp.where(sub, packed[0], packed[1]).astype(BF16)
        for t in range(STRIDE, 0, -1):
            returning(slot_of(m, True, t), -(m * STRIDE + t))
            if m < l_groups and slot_of(m, False, t) != last:
                returning(slot_of(m, False, t), m * STRIDE + t)
    res[z] = sbuf[last]

    for dz in range(1, nz):
        src = chip(dz)
        remote(res.at[src], res.at[src], rsend.at[0], rrecv.at[src], partner).wait_recv()

    row = lax.broadcasted_iota(jnp.int32, (8, 128), 0)
    lane = lax.broadcasted_iota(jnp.int32, (8, 128), 1)
    col = (row // 4) * 128 + lane
    segments = nz // STRIDE
    acc = [jnp.zeros((8, 128), F32) for _ in range(segments)]
    for rho in range(STRIDE):
        gap = (col // 64 - rho + STRIDE) & (STRIDE - 1)
        shift = jnp.where(gap == 3, -1, gap)
        shift = jnp.where(gap == 2, jnp.where((col // 32) % 2 == 0, -2, 2), shift)
        target = rho + shift
        seg_masks = {-1: target < 0, 0: (target >= 0) & (target < STRIDE), 1: target >= STRIDE}
        used = {0} | ({-1} if rho < 2 else set()) | ({1} if rho >= STRIDE - 2 else set())
        for s in range(segments):
            val = res[s * STRIDE + rho].astype(F32)
            for rel in sorted(used):
                to = (s + rel) % segments
                acc[to] = acc[to] + jnp.where(seg_masks[rel], val, 0.0)
    for s in range(segments):
        out[:, s * 256 : s * 256 + 128] = acc[s][:4].astype(out.dtype)
        out[:, s * 256 + 128 : s * 256 + 256] = acc[s][4:].astype(out.dtype)

    for cp in q_sends + passed + ups + downs + forwards + returns:
        cp.wait_send()


def local(nz, activations, out_grads, lengths, proj_in, proj_out, queries):
    toks, ff = activations.shape
    d = out_grads.shape[1]
    rank = proj_in.shape[1]
    nq, params = queries.shape
    chunk = min(2048, d)
    n_loc = 1 + len(cuts(d, chunk)) + 2 * len(cuts(ff, chunk))
    dma = pltpu.SemaphoreType.DMA
    anyspec = pl.BlockSpec(memory_space=pl.ANY)
    rows = rank // STRIDE
    return pl.pallas_call(
        functools.partial(kernel, nz, chunk),
        out_shape=jax.ShapeDtypeStruct((lengths.shape[1], 2 * nz * nq), BF16),
        in_specs=[
            anyspec, anyspec, pl.BlockSpec(memory_space=pltpu.SMEM), anyspec, anyspec, anyspec,
        ],
        out_specs=pl.BlockSpec(memory_space=pltpu.VMEM),
        scratch_shapes=[
            pltpu.VMEM((toks, ff), BF16),
            pltpu.VMEM((toks, d), BF16),
            pltpu.VMEM((rank, ff), BF16),
            pltpu.VMEM((rank, d), BF16),
            pltpu.VMEM((nq, params), BF16),
            pltpu.VMEM((2 * STRIDE, nq, params // STRIDE), BF16),
            pltpu.VMEM((STRIDE, rows, 4 * rank), BF16),
            pltpu.VMEM((nz, rows, 4 * rank), BF16),
            pltpu.VMEM((nz, 8, 128), BF16),
            pltpu.VMEM((nz, 8, 128), BF16),
            dma((n_loc,)), dma((2,)), dma((7,)), dma((7,)), dma((2 * STRIDE,)),
            dma((nz,)), dma((nz,)), dma((nz,)), dma((nz,)), pltpu.SemaphoreType.REGULAR,
        ],
        compiler_params=pltpu.CompilerParams(collective_id=0, has_side_effects=True),
        name="score",
    )(activations, out_grads, lengths, proj_in.T, proj_out.T, queries)


def solution(mesh):
    both = P(("parts", "dp"), None)
    in_specs = (both, both, both, P(), P(), both)
    body = functools.partial(local, mesh.shape["dp"] // 2)
    return jax.shard_map(body, mesh=mesh, in_specs=in_specs, out_specs=both, check_vma=False)
```

```python
import functools

import jax
import jax.numpy as jnp
from jax import lax
from jax.experimental import pallas as pl
from jax.experimental.pallas import tpu as pltpu
from jax.sharding import PartitionSpec as P

MESH = pl.DeviceIdType.MESH
STRIDE = 4
F32 = jnp.float32
BF16 = jnp.bfloat16
NT = (((1,), (1,)), ((), ()))


def cuts(total, size):
    widths = [size] * (total // size)
    if total % size:
        widths.append(total % size)
    if widths[-1] % 256 == 0 and widths[-1] >= 512:
        widths[-1:] = [widths[-1] // 2] * 2
    starts = [sum(widths[:i]) for i in range(len(widths))]
    return list(zip(starts, widths))


def split(nz):
    total = nz // STRIDE
    return total - total // 2, total // 2


def kernel(
    nz, chunk, acts, grads, lens, pin, pout, qs, out,
    abuf, gbuf, pinb, poutb, qv, qbuf, ybuf, rbuf, sbuf, res,
    loc_sem, qloc_sem, qsend, qrecv, dsend, fsend, erecv, rsend, rrecv, wrap_sem, pg_sum, pa_sum,
):
    me = lax.axis_index("dp")
    z, core = me // 2, lax.rem(me, 2)
    part = lax.rem(z, STRIDE)
    r_groups, l_groups = split(nz)
    toks, ff = acts.shape
    d = grads.shape[1]
    rank = pin.shape[0]
    kq = qs.shape[1] // STRIDE

    def chip(dz):
        return lax.rem(z + nz + dz, nz)

    def dev(dz):
        return {"dp": chip(dz) * 2 + core}

    partner = {"dp": z * 2 + 1 - core}

    def remote(src, dst, ssem, rsem, to):
        return pltpu.make_async_remote_copy(
            src_ref=src, dst_ref=dst, send_sem=ssem, recv_sem=rsem,
            device_id=to, device_id_type=MESH,
        )

    def q_cols(dz):
        return pl.ds(pl.multiple_of(lax.rem(z + nz + dz, STRIDE) * kq, kq), kq)

    n_sem = 0
    g_chunks, a_chunks = [], []
    pout_copy = pltpu.make_async_copy(pout, poutb, loc_sem.at[n_sem])
    pout_copy.start()
    n_sem += 1
    for lo, w in cuts(d, chunk):
        cp = pltpu.make_async_copy(
            grads.at[:, pl.ds(lo, w)], gbuf.at[:, pl.ds(lo, w)], loc_sem.at[n_sem]
        )
        cp.start()
        n_sem += 1
        g_chunks.append((lo, w, cp))
    q_all = pltpu.make_async_copy(qs, qv, qloc_sem.at[0])
    q_own = pltpu.make_async_copy(qs.at[:, q_cols(0)], qbuf.at[part * 2 + core], qloc_sem.at[1])
    q_all.start()
    q_own.start()
    for lo, w in cuts(ff, chunk):
        cp0 = pltpu.make_async_copy(
            pin.at[:, pl.ds(lo, w)], pinb.at[:, pl.ds(lo, w)], loc_sem.at[n_sem]
        )
        cp1 = pltpu.make_async_copy(
            acts.at[:, pl.ds(lo, w)], abuf.at[:, pl.ds(lo, w)], loc_sem.at[n_sem + 1]
        )
        cp0.start()
        cp1.start()
        n_sem += 2
        a_chunks.append((lo, w, cp0, cp1))

    barrier = pltpu.get_barrier_semaphore()
    near = [dz for t in range(1, STRIDE + 1) for dz in (t, -t)]

    def greet(sem, dz):
        pl.semaphore_signal(sem, inc=1, device_id=dev(dz), device_id_type=MESH)

    for dz in near:
        if dz < 0:
            greet(barrier, dz)
        else:
            pl.when(z + dz < nz)(functools.partial(greet, barrier, dz))
    pl.semaphore_signal(barrier, inc=1, device_id=partner, device_id_type=MESH)

    def await_near():
        pl.semaphore_wait(barrier, len(near) + 1 - jnp.maximum(STRIDE - z, 0))
        for dz in range(1, STRIDE + 1):
            pl.when(z + dz >= nz)(functools.partial(greet, wrap_sem, dz))

    def add_product(x_ref, w_ref, lo, w, total, copies):
        for i in range(2):
            cols = slice(lo + i * (w // 2), lo + (i + 1) * (w // 2))
            p = w_ref[:, cols]
            p = jnp.concatenate([p] * copies, axis=0) if copies > 1 else p
            prod = lax.dot_general(x_ref[:, cols], p, NT, preferred_element_type=F32)
            width = prod.shape[1]
            if lo == 0:
                total[i, :, :width] = prod
            else:
                total[i, :, :width] += prod

    pout_copy.wait()
    for lo, w, cp in g_chunks:
        cp.wait()
        add_product(gbuf, poutb, lo, w, pg_sum, 1)
    pg = (pg_sum[0, :, :rank] + pg_sum[1, :, :rank]).astype(BF16)
    rows = 4 * rank
    r = lax.broadcasted_iota(jnp.int32, (rows, rank), 0)
    i = lax.broadcasted_iota(jnp.int32, (rows, rank), 1)
    quarter = r // rank
    i_lo = (quarter & 1) * 2 + quarter // 2
    spread = (i == ((r & (rank - 1)) & ~3) + i_lo).astype(F32).astype(BF16)
    wide = lax.dot_general(spread, pg, NT, preferred_element_type=F32)
    e = lax.broadcasted_iota(jnp.int32, (8, toks), 0) & 3
    tok = lax.broadcasted_iota(jnp.int32, (8, toks), 1)
    end0 = lens[0, 0]
    end1 = end0 + lens[0, 1]
    end2 = end1 + lens[0, 2]
    owner = (
        (tok >= end0).astype(jnp.int32)
        + (tok >= end1).astype(jnp.int32)
        + (tok >= end2).astype(jnp.int32)
    )
    member = (owner == e)[None]
    lhs = jnp.where(member, wide.reshape(rows // 8, 8, toks), 0.0).reshape(rows, toks).astype(BF16)

    slot = part * 2 + core
    q_up = remote(qv.at[:, q_cols(1)], qbuf.at[slot], qsend.at[0], qrecv.at[0], dev(1))
    q_down = remote(qv.at[:, q_cols(-1)], qbuf.at[slot], qsend.at[1], qrecv.at[1], dev(-1))
    far = {"dp": lax.rem(z + nz + 2 - 4 * core, nz) * 2 + core}
    q_far = remote(qv.at[:, q_cols(2)], qbuf.at[slot], qsend.at[2], qrecv.at[2], far)
    q_near = remote(qv.at[:, q_cols(0)], qbuf.at[slot], qsend.at[3], qrecv.at[3], partner)
    q_sends = [q_up, q_down, q_far, q_near]
    for n, (lo, w, cp0, cp1) in enumerate(a_chunks):
        if n == min(2, len(a_chunks) - 1):
            q_all.wait()
            await_near()
            q_up.start()
            q_near.start()
            pl.when((z >= STRIDE) | (core == 0))(q_far.start)
            pl.when(z >= STRIDE)(q_down.start)
        cp0.wait()
        cp1.wait()
        add_product(abuf, pinb, lo, w, pa_sum, 2)
    pa = pa_sum[0] + pa_sum[1]
    left = lax.broadcasted_iota(jnp.int32, (toks, 2 * rank), 1) < rank
    pa_l = jnp.where(left, pa, 0.0).astype(BF16)
    pa_r = jnp.where(left, 0.0, pa).astype(BF16)
    half = 2 * rank
    y = jnp.dot(lhs[:half], pa_l, preferred_element_type=F32) + jnp.dot(
        lhs[half:], pa_r, preferred_element_type=F32
    )
    y = jnp.concatenate([y[:rank], y[rank:]], axis=1).astype(BF16)
    own_rows = rank // STRIDE
    for s in range(STRIDE):
        ybuf[s] = y[s * own_rows : (s + 1) * own_rows]

    quads = nz // STRIDE
    quad = z // STRIDE

    def slot_of(source):
        return lax.rem(quad + quads - source // STRIDE, quads) * STRIDE + lax.rem(source, STRIDE)

    def leg(up, t):
        dz = t if up else -t
        k = lax.rem(chip(dz) // STRIDE + quads - quad, quads) * STRIDE + part
        i = (0 if up else STRIDE) + t - 1
        return remote(
            ybuf.at[lax.rem(z + nz + dz, STRIDE)], rbuf.at[k], dsend.at[i], erecv.at[k], dev(dz)
        )

    hops = range(STRIDE, 0, -1)
    ups = [leg(True, t) for t in hops]
    downs = [leg(False, t) for t in hops if l_groups > 1 or t < STRIDE]
    for cp in ups:
        cp.start()

    def start_downs():
        for cp in downs:
            cp.start()

    def after_wrap():
        pl.semaphore_wait(wrap_sem, STRIDE - z)
        q_down.start()
        pl.when(core == 1)(q_far.start)
        start_downs()

    pl.when(z >= STRIDE)(start_downs)
    rbuf[part] = ybuf[part]
    q_own.wait()

    up_reach, down_reach = r_groups * STRIDE, l_groups * STRIDE - 1

    def onward(k, up):
        nxt = lax.rem(k + (STRIDE if up else nz - STRIDE), nz)
        return remote(
            rbuf.at[k], rbuf.at[nxt], fsend.at[k], erecv.at[nxt], dev(STRIDE if up else -STRIDE)
        )

    def take(i, up):
        k = slot_of(chip(-i if up else i))
        remote(rbuf.at[k], rbuf.at[k], fsend.at[k], erecv.at[k], partner).wait_recv()
        if i + STRIDE <= (up_reach if up else down_reach):
            onward(k, up).start()

    def step_of(source):
        up = lax.rem(z + nz - source, nz)
        away = jnp.where(up <= up_reach, up, nz - up)
        return jnp.where(up == 0, 0, (away - 1) // STRIDE)

    def source_of(g, i):
        return lax.rem(quad + quads - g, quads) * STRIDE + i

    def back(g, i):
        k = g * STRIDE + i
        to = {"dp": source_of(g, i) * 2 + core}
        return remote(sbuf.at[k], res.at[z], rsend.at[k], rrecv.at[z], to)

    sub = lax.broadcasted_iota(jnp.int32, (STRIDE, 8, 128), 1) < 4

    def score(g):
        held = rbuf[pl.ds(g * STRIDE, STRIDE)].reshape(STRIDE * own_rows, 4 * rank)
        prods = []
        for i in range(STRIDE):
            w = qbuf[:, :, i * 256 : (i + 1) * 256].reshape(-1, 256)
            pr = lax.dot_general(held, w, NT, preferred_element_type=F32)
            pr = pr.reshape(STRIDE, own_rows, pr.shape[-1])
            prods.append(pr[:, 8 * (i // 2) : 8 * (i // 2) + 8])
        packed = []
        for h in range(2):
            c0, c1 = h * 128, (h + 1) * 128
            s = jnp.where(sub, prods[0][:, :, c0:c1], prods[1][:, :, c0:c1])
            s = s + jnp.where(sub, prods[2][:, :, c0:c1], prods[3][:, :, c0:c1])
            packed.append(s + pltpu.roll(s, 4, 1))
        sbuf[pl.ds(g * STRIDE, STRIDE)] = jnp.where(sub, packed[0], packed[1]).astype(BF16)

        def send(i, carry):
            pl.when(source_of(g, i) != z)(lambda: back(g, i).start())
            return carry

        lax.fori_loop(0, STRIDE, send, 0)

    def score_step(step):
        def visit(g, carry):
            done = jnp.maximum(step_of(source_of(g, 0)), step_of(source_of(g, STRIDE - 1)))
            pl.when(done == step)(lambda: score(g))
            return carry

        lax.fori_loop(0, quads, visit, 0)

    passed = []
    for step in range(r_groups):
        for t in range(1, STRIDE + 1):
            if step == 0:
                pl.when(z == t - 1)(after_wrap)
            take(step * STRIDE + t, True)
        if step == 0:
            for k, dz in enumerate((-1, 1, 2)):
                came = lax.rem(z + nz + dz, STRIDE) * 2 + core
                q_sends[k].wait_recv()
                passed.append(
                    remote(
                        qbuf.at[came], qbuf.at[came], qsend.at[4 + k], qrecv.at[4 + k], partner
                    )
                )
                passed[-1].start()
        for t in range(1, STRIDE + 1):
            if step * STRIDE + t <= down_reach:
                take(step * STRIDE + t, False)
        if step == 0:
            q_near.wait_recv()
            for cp in passed:
                cp.wait_recv()
        score_step(step)
    res[z] = sbuf[part]

    for cp in q_sends + passed + ups + downs:
        cp.wait_send()

    def settle(i, carry):
        source = chip(-i)
        k = slot_of(source)
        pl.when(i + STRIDE <= up_reach)(lambda: onward(k, True).wait_send())
        pl.when((nz - i) + STRIDE <= down_reach)(lambda: onward(k, False).wait_send())
        back(k // STRIDE, lax.rem(k, STRIDE)).wait_send()
        return carry

    lax.fori_loop(1, nz, settle, 0)

    def collect(dz, carry):
        src = chip(dz)
        remote(res.at[src], res.at[src], rsend.at[0], rrecv.at[src], partner).wait_recv()
        return carry

    lax.fori_loop(1, nz, collect, 0)

    row = lax.broadcasted_iota(jnp.int32, (8, 128), 0)
    lane = lax.broadcasted_iota(jnp.int32, (8, 128), 1)
    col = (row // 4) * 128 + lane
    masks = []
    for rho in range(STRIDE):
        gap = (col // 64 - rho + STRIDE) & (STRIDE - 1)
        shift = jnp.where(gap == 3, -1, gap)
        shift = jnp.where(gap == 2, jnp.where((col // 32) % 2 == 0, -2, 2), shift)
        target = rho + shift
        masks.append((rho, 0, (target >= 0) & (target < STRIDE)))
        if rho < 2:
            masks.append((rho, -1, target < 0))
        else:
            masks.append((rho, 1, target >= STRIDE))

    def add_up(seg, carry):
        total = jnp.zeros((8, 128), F32)
        for rho, rel, mask in masks:
            val = res[lax.rem(seg + quads - rel, quads) * STRIDE + rho].astype(F32)
            total = total + jnp.where(mask, val, 0.0)
        out[seg] = total.astype(out.dtype)
        return carry

    lax.fori_loop(0, quads, add_up, 0)


def local(nz, activations, out_grads, lengths, proj_in, proj_out, queries):
    toks, ff = activations.shape
    d = out_grads.shape[1]
    rank = proj_in.shape[1]
    nq, params = queries.shape
    chunk = min(2048, d)
    n_loc = 1 + len(cuts(d, chunk)) + 2 * len(cuts(ff, chunk))
    dma = pltpu.SemaphoreType.DMA
    anyspec = pl.BlockSpec(memory_space=pl.ANY)
    rows = rank // STRIDE
    scores = pl.pallas_call(
        functools.partial(kernel, nz, chunk),
        out_shape=jax.ShapeDtypeStruct((nz // STRIDE, 8, 128), BF16),
        in_specs=[
            anyspec, anyspec, pl.BlockSpec(memory_space=pltpu.SMEM), anyspec, anyspec, anyspec,
        ],
        out_specs=pl.BlockSpec(memory_space=pltpu.VMEM),
        scratch_shapes=[
            pltpu.VMEM((toks, ff), BF16),
            pltpu.VMEM((toks, d), BF16),
            pltpu.VMEM((rank, ff), BF16),
            pltpu.VMEM((rank, d), BF16),
            pltpu.VMEM((nq, params), BF16),
            pltpu.VMEM((2 * STRIDE, nq, params // STRIDE), BF16),
            pltpu.VMEM((STRIDE, rows, 4 * rank), BF16),
            pltpu.VMEM((nz, rows, 4 * rank), BF16),
            pltpu.VMEM((nz, 8, 128), BF16),
            pltpu.VMEM((nz, 8, 128), BF16),
            dma((n_loc,)), dma((2,)), dma((7,)), dma((7,)), dma((2 * STRIDE,)),
            dma((nz,)), dma((nz,)), dma((nz,)), dma((nz,)), pltpu.SemaphoreType.REGULAR,
            pltpu.VMEM((2, toks, 2 * rank), F32),
            pltpu.VMEM((2, toks, 2 * rank), F32),
        ],
        compiler_params=pltpu.CompilerParams(collective_id=0, has_side_effects=True),
        name="score",
    )(activations, out_grads, lengths, proj_in.T, proj_out.T, queries)
    scores = scores.reshape(nz // STRIDE, 2, 4, 128).transpose(2, 0, 1, 3)
    return scores.reshape(lengths.shape[1], 2 * nz * nq)


def solution(mesh):
    both = P(("parts", "dp"), None)
    in_specs = (both, both, both, P(), P(), both)
    body = functools.partial(local, mesh.shape["dp"] // 2)
    return jax.shard_map(body, mesh=mesh, in_specs=in_specs, out_specs=both, check_vma=False)
```

```python
import functools

import jax
import jax.numpy as jnp
from jax import lax
from jax.experimental import pallas as pl
from jax.experimental.pallas import tpu as pltpu
from jax.sharding import PartitionSpec as P

MESH = pl.DeviceIdType.MESH
STRIDE = 4
F32 = jnp.float32
BF16 = jnp.bfloat16
NT = (((1,), (1,)), ((), ()))


def cuts(total, size):
    widths = [size] * (total // size)
    if total % size:
        widths.append(total % size)
    if widths[-1] % 256 == 0 and widths[-1] >= 512:
        widths[-1:] = [widths[-1] // 2] * 2
    starts = [sum(widths[:i]) for i in range(len(widths))]
    return list(zip(starts, widths))


def kernel(
    nz, chunk, acts, grads, lens, pin, pout, qs, out,
    abuf, gbuf, pinb, poutb, qbuf, ybuf, rbuf, sbuf, res,
    loc_sem, qloc_sem, qsend, qrecv, dsend, fsend, erecv, rsend, rrecv, wrap_sem, pg_sum, pa_sum,
):
    me = lax.axis_index("dp")
    z, core = me // 2, lax.rem(me, 2)
    part = lax.rem(z, STRIDE)
    toks, ff = acts.shape
    d = grads.shape[1]
    rank = pin.shape[0]
    kq = qs.shape[1] // STRIDE

    def chip(dz):
        return lax.rem(z + nz + dz, nz)

    def dev(dz):
        return {"dp": chip(dz) * 2 + core}

    partner = {"dp": z * 2 + 1 - core}

    def remote(src, dst, ssem, rsem, to):
        return pltpu.make_async_remote_copy(
            src_ref=src, dst_ref=dst, send_sem=ssem, recv_sem=rsem,
            device_id=to, device_id_type=MESH,
        )

    def q_cols(dz):
        return pl.ds(pl.multiple_of(lax.rem(z + nz + dz, STRIDE) * kq, kq), kq)

    n_sem = 0
    g_chunks, a_chunks = [], []
    pout_copy = pltpu.make_async_copy(pout, poutb, loc_sem.at[n_sem])
    pout_copy.start()
    n_sem += 1
    for lo, w in cuts(d, chunk):
        cp = pltpu.make_async_copy(
            grads.at[:, pl.ds(lo, w)], gbuf.at[:, pl.ds(lo, w)], loc_sem.at[n_sem]
        )
        cp.start()
        n_sem += 1
        g_chunks.append((lo, w, cp))
    q_own = pltpu.make_async_copy(qs.at[:, q_cols(0)], qbuf.at[part * 2 + core], qloc_sem)
    q_own.start()
    pieces = cuts(ff, chunk)
    middle = pieces[len(pieces) // 2][0]
    halves = {0: slice(0, middle), middle: slice(middle, ff)}
    for lo, w in pieces:
        waits = []
        if lo in halves:
            cols = halves[lo]
            waits.append(
                pltpu.make_async_copy(pin.at[:, cols], pinb.at[:, cols], loc_sem.at[n_sem])
            )
            n_sem += 1
        waits.append(
            pltpu.make_async_copy(
                acts.at[:, pl.ds(lo, w)], abuf.at[:, pl.ds(lo, w)], loc_sem.at[n_sem]
            )
        )
        n_sem += 1
        for cp in waits:
            cp.start()
        a_chunks.append((lo, w, waits))

    barrier = pltpu.get_barrier_semaphore()
    near = [dz for t in range(1, STRIDE + 1) for dz in (t, -t)]

    def greet(sem, dz):
        pl.semaphore_signal(sem, inc=1, device_id=dev(dz), device_id_type=MESH)

    for dz in near:
        if dz < 0:
            greet(barrier, dz)
        else:
            pl.when(z + dz < nz)(functools.partial(greet, barrier, dz))
    pl.semaphore_signal(barrier, inc=1, device_id=partner, device_id_type=MESH)

    def await_near():
        pl.semaphore_wait(barrier, len(near) + 1 - jnp.maximum(STRIDE - z, 0))
        for dz in range(1, STRIDE + 1):
            pl.when(z + dz >= nz)(functools.partial(greet, wrap_sem, dz))

    def add_product(x_ref, w_ref, lo, w, total, copies):
        for i in range(2):
            cols = slice(lo + i * (w // 2), lo + (i + 1) * (w // 2))
            p = w_ref[:, cols]
            p = jnp.concatenate([p] * copies, axis=0) if copies > 1 else p
            prod = lax.dot_general(x_ref[:, cols], p, NT, preferred_element_type=F32)
            width = prod.shape[1]
            if lo == 0:
                total[i, :, :width] = prod
            else:
                total[i, :, :width] += prod

    pout_copy.wait()
    for lo, w, cp in g_chunks:
        cp.wait()
        add_product(gbuf, poutb, lo, w, pg_sum, 1)
    pg = (pg_sum[0, :, :rank] + pg_sum[1, :, :rank]).astype(BF16)
    rows = 4 * rank
    r = lax.broadcasted_iota(jnp.int32, (rows, rank), 0)
    i = lax.broadcasted_iota(jnp.int32, (rows, rank), 1)
    quarter = r // rank
    i_lo = (quarter & 1) * 2 + quarter // 2
    spread = (i == ((r & (rank - 1)) & ~3) + i_lo).astype(F32).astype(BF16)
    wide = lax.dot_general(spread, pg, NT, preferred_element_type=F32)
    e = lax.broadcasted_iota(jnp.int32, (8, toks), 0) & 3
    tok = lax.broadcasted_iota(jnp.int32, (8, toks), 1)
    end0 = lens[0, 0]
    end1 = end0 + lens[0, 1]
    end2 = end1 + lens[0, 2]
    owner = (
        (tok >= end0).astype(jnp.int32)
        + (tok >= end1).astype(jnp.int32)
        + (tok >= end2).astype(jnp.int32)
    )
    member = (owner == e)[None]
    lhs = jnp.where(member, wide.reshape(rows // 8, 8, toks), 0.0).reshape(rows, toks).astype(BF16)

    slot = part * 2 + core
    q_up = remote(qs.at[:, q_cols(1)], qbuf.at[slot], qsend, qrecv.at[0], dev(1))
    q_down = remote(qs.at[:, q_cols(-1)], qbuf.at[slot], qsend, qrecv.at[1], dev(-1))
    far = {"dp": lax.rem(z + nz + 2 - 4 * core, nz) * 2 + core}
    q_far = remote(qs.at[:, q_cols(2)], qbuf.at[slot], qsend, qrecv.at[2], far)
    q_near = remote(qs.at[:, q_cols(0)], qbuf.at[slot], qsend, qrecv.at[3], partner)
    q_sends = [q_up, q_down, q_far, q_near]
    for n, (lo, w, waits) in enumerate(a_chunks):
        if n == min(1, len(a_chunks) - 1):
            await_near()
            q_up.start()
            q_near.start()
            pl.when((z >= STRIDE) | (core == 0))(q_far.start)
            pl.when(z >= STRIDE)(q_down.start)
        for cp in waits:
            cp.wait()
        add_product(abuf, pinb, lo, w, pa_sum, 2)
    pa = pa_sum[0] + pa_sum[1]
    left = lax.broadcasted_iota(jnp.int32, (toks, 2 * rank), 1) < rank
    pa_l = jnp.where(left, pa, 0.0).astype(BF16)
    pa_r = jnp.where(left, 0.0, pa).astype(BF16)
    half = 2 * rank
    y = jnp.dot(lhs[:half], pa_l, preferred_element_type=F32) + jnp.dot(
        lhs[half:], pa_r, preferred_element_type=F32
    )
    y = jnp.concatenate([y[:rank], y[rank:]], axis=1).astype(BF16)
    own_rows = rank // STRIDE
    for s in range(STRIDE):
        ybuf[s] = y[s * own_rows : (s + 1) * own_rows]

    groups, blocks = nz // (2 * STRIDE), 2 * STRIDE
    own = nz - 1

    def slot_of(i, up):
        return (i - 1) // STRIDE * blocks + (0 if up else STRIDE) + (i - 1) % STRIDE

    def leg(up, t):
        dz = t if up else -t
        k = slot_of(t, up)
        return remote(
            ybuf.at[lax.rem(z + nz + dz, STRIDE)], rbuf.at[k], dsend, erecv.at[k], dev(dz)
        )

    hops = range(STRIDE, 0, -1)
    ups = [leg(True, t) for t in hops]
    downs = [leg(False, t) for t in hops if slot_of(t, False) != own]
    for cp in ups:
        cp.start()

    def start_downs():
        for cp in downs:
            cp.start()

    def after_wrap():
        pl.semaphore_wait(wrap_sem, STRIDE - z)
        start_downs()
        q_down.start()
        pl.when(core == 1)(q_far.start)

    pl.when(z >= STRIDE)(start_downs)
    rbuf[own] = ybuf[part]
    q_own.wait()

    def take(i, up):
        k = slot_of(i, up)
        remote(rbuf.at[k], rbuf.at[k], fsend, erecv.at[k], partner).wait_recv()
        nxt = k + blocks
        if nxt < own:
            remote(
                rbuf.at[k], rbuf.at[nxt], fsend, erecv.at[nxt],
                dev(STRIDE if up else -STRIDE),
            ).start()

    sub = lax.broadcasted_iota(jnp.int32, (blocks, 8, 128), 1) < 4

    def back(k, dz):
        return remote(sbuf.at[k], res.at[z], rsend, rrecv, dev(dz))

    def score(step):
        slots = slice(step * blocks, (step + 1) * blocks)
        held = rbuf[slots].reshape(blocks * own_rows, 4 * rank)
        prods = []
        for i in range(STRIDE):
            w = qbuf[:, :, i * 256 : (i + 1) * 256].reshape(-1, 256)
            pr = lax.dot_general(held, w, NT, preferred_element_type=F32)
            pr = pr.reshape(blocks, own_rows, pr.shape[-1])
            prods.append(pr[:, 8 * (i // 2) : 8 * (i // 2) + 8])
        packed = []
        for h in range(2):
            c0, c1 = h * 128, (h + 1) * 128
            s = jnp.where(sub, prods[0][:, :, c0:c1], prods[1][:, :, c0:c1])
            s = s + jnp.where(sub, prods[2][:, :, c0:c1], prods[3][:, :, c0:c1])
            packed.append(s + pltpu.roll(s, 4, 1))
        sbuf[slots] = jnp.where(sub, packed[0], packed[1]).astype(BF16)
        for t in range(STRIDE, 0, -1):
            i = step * STRIDE + t
            back(slot_of(i, True), -i).start()
            if slot_of(i, False) != own:
                back(slot_of(i, False), i).start()

    passed = []
    for step in range(groups):
        for t in range(1, STRIDE + 1):
            if step == 0:
                pl.when(z == t - 1)(after_wrap)
            take(step * STRIDE + t, True)
        if step == 0:
            for k, dz in enumerate((-1, 1, 2)):
                came = lax.rem(z + nz + dz, STRIDE) * 2 + core
                q_sends[k].wait_recv()
                passed.append(
                    remote(
                        qbuf.at[came], qbuf.at[came], qsend, qrecv.at[4 + k], partner
                    )
                )
                passed[-1].start()
        for t in range(1, STRIDE + 1):
            if slot_of(step * STRIDE + t, False) != own:
                take(step * STRIDE + t, False)
        if step == 0:
            q_near.wait_recv()
            for cp in passed:
                cp.wait_recv()
        score(step)
    res[z] = sbuf[own]

    def sent(ref, count, sem):
        many = ref.at[pl.ds(0, count)]
        remote(many, many, sem, rrecv, partner).wait_send()

    sent(qbuf, len(q_sends) + len(passed), qsend)
    sent(rbuf, len(ups) + len(downs), dsend)
    if own > blocks:
        sent(rbuf, own - blocks, fsend)
    sent(sbuf, own, rsend)
    others = res.at[pl.ds(0, own)]
    remote(others, others, rsend, rrecv, partner).wait_recv()

    quads = nz // STRIDE
    row = lax.broadcasted_iota(jnp.int32, (8, 128), 0)
    lane = lax.broadcasted_iota(jnp.int32, (8, 128), 1)
    col = (row // 4) * 128 + lane
    masks = []
    for rho in range(STRIDE):
        gap = (col // 64 - rho + STRIDE) & (STRIDE - 1)
        shift = jnp.where(gap == 3, -1, gap)
        shift = jnp.where(gap == 2, jnp.where((col // 32) % 2 == 0, -2, 2), shift)
        target = rho + shift
        masks.append((rho, 0, (target >= 0) & (target < STRIDE)))
        if rho < 2:
            masks.append((rho, -1, target < 0))
        else:
            masks.append((rho, 1, target >= STRIDE))

    def add_up(seg, carry):
        total = jnp.zeros((8, 128), F32)
        for rho, rel, mask in masks:
            val = res[lax.rem(seg + quads - rel, quads) * STRIDE + rho].astype(F32)
            total = total + jnp.where(mask, val, 0.0)
        out[seg] = total.astype(out.dtype)
        return carry

    lax.fori_loop(0, quads, add_up, 0)


def local(nz, activations, out_grads, lengths, proj_in, proj_out, queries):
    toks, ff = activations.shape
    d = out_grads.shape[1]
    rank = proj_in.shape[1]
    nq, params = queries.shape
    chunk = min(2048, d)
    n_loc = 3 + len(cuts(d, chunk)) + len(cuts(ff, chunk))
    dma = pltpu.SemaphoreType.DMA
    anyspec = pl.BlockSpec(memory_space=pl.ANY)
    rows = rank // STRIDE
    scores = pl.pallas_call(
        functools.partial(kernel, nz, chunk),
        out_shape=jax.ShapeDtypeStruct((nz // STRIDE, 8, 128), BF16),
        in_specs=[
            anyspec, anyspec, pl.BlockSpec(memory_space=pltpu.SMEM), anyspec, anyspec, anyspec,
        ],
        out_specs=pl.BlockSpec(memory_space=pltpu.VMEM),
        scratch_shapes=[
            pltpu.VMEM((toks, ff), BF16),
            pltpu.VMEM((toks, d), BF16),
            pltpu.VMEM((rank, ff), BF16),
            pltpu.VMEM((rank, d), BF16),
            pltpu.VMEM((2 * STRIDE, nq, params // STRIDE), BF16),
            pltpu.VMEM((STRIDE, rows, 4 * rank), BF16),
            pltpu.VMEM((nz, rows, 4 * rank), BF16),
            pltpu.VMEM((nz, 8, 128), BF16),
            pltpu.VMEM((nz, 8, 128), BF16),
            dma((n_loc,)), dma(()), dma(()), dma((7,)), dma(()),
            dma(()), dma((nz,)), dma(()), dma(()), pltpu.SemaphoreType.REGULAR,
            pltpu.VMEM((2, toks, 2 * rank), F32),
            pltpu.VMEM((2, toks, 2 * rank), F32),
        ],
        compiler_params=pltpu.CompilerParams(collective_id=0, has_side_effects=True),
        name="score",
    )(activations, out_grads, lengths, proj_in.T, proj_out.T, queries)
    scores = scores.reshape(nz // STRIDE, 2, 4, 128).transpose(2, 0, 1, 3)
    return scores.reshape(lengths.shape[1], 2 * nz * nq)


def solution(mesh):
    both = P(("parts", "dp"), None)
    in_specs = (both, both, both, P(), P(), both)
    body = functools.partial(local, mesh.shape["dp"] // 2)
    return jax.shard_map(body, mesh=mesh, in_specs=in_specs, out_specs=both, check_vma=False)
```

```python
import functools

import jax
import jax.numpy as jnp
from jax import lax
from jax.experimental import pallas as pl
from jax.experimental.pallas import tpu as pltpu
from jax.sharding import PartitionSpec as P

MESH = pl.DeviceIdType.MESH
STRIDE = 4
F32 = jnp.float32
BF16 = jnp.bfloat16
NT = (((1,), (1,)), ((), ()))


def cuts(total, size):
    widths = [size] * (total // size)
    if total % size:
        widths.append(total % size)
    if widths[-1] % 256 == 0 and widths[-1] >= 512:
        widths[-1:] = [widths[-1] // 2] * 2
    starts = [sum(widths[:i]) for i in range(len(widths))]
    return list(zip(starts, widths))


def kernel(
    nz, chunk, acts, grads, lens, pin, pout, qs, out,
    abuf, gbuf, pinb, poutb, qbuf, ybuf, rbuf, sbuf, res,
    loc_sem, qloc_sem, qsend, qrecv, dsend, fsend, erecv, rsend, rrecv, wrap_sem, pg_sum, pa_sum,
):
    me = lax.axis_index("dp")
    z, core = me // 2, lax.rem(me, 2)
    part = lax.rem(z, STRIDE)
    toks, ff = acts.shape
    d = grads.shape[1]
    rank = pin.shape[0]
    kq = qs.shape[1] // STRIDE

    def chip(dz):
        return lax.rem(z + nz + dz, nz)

    def dev(dz, c=1):
        return {"dp": chip(dz) * 2 + c}

    relays = core == 1

    partner = {"dp": z * 2 + 1 - core}

    def remote(src, dst, ssem, rsem, to):
        return pltpu.make_async_remote_copy(
            src_ref=src, dst_ref=dst, send_sem=ssem, recv_sem=rsem,
            device_id=to, device_id_type=MESH,
        )

    def q_cols(dz):
        return pl.ds(pl.multiple_of(lax.rem(z + nz + dz, STRIDE) * kq, kq), kq)

    n_sem = 0
    g_chunks, a_chunks = [], []
    pout_copy = pltpu.make_async_copy(pout, poutb, loc_sem.at[n_sem])
    pout_copy.start()
    n_sem += 1
    for lo, w in cuts(d, chunk):
        cp = pltpu.make_async_copy(
            grads.at[:, pl.ds(lo, w)], gbuf.at[:, pl.ds(lo, w)], loc_sem.at[n_sem]
        )
        cp.start()
        n_sem += 1
        g_chunks.append((lo, w, cp))
    q_own = pltpu.make_async_copy(qs.at[:, q_cols(0)], qbuf.at[part * 2 + core], qloc_sem)
    pl.when(core == 1)(q_own.start)
    pieces = cuts(ff, chunk)
    middle = pieces[len(pieces) // 2][0]
    halves = {0: slice(0, middle), middle: slice(middle, ff)}
    for lo, w in pieces:
        waits = []
        if lo in halves:
            cols = halves[lo]
            waits.append(
                pltpu.make_async_copy(pin.at[:, cols], pinb.at[:, cols], loc_sem.at[n_sem])
            )
            n_sem += 1
        waits.append(
            pltpu.make_async_copy(
                acts.at[:, pl.ds(lo, w)], abuf.at[:, pl.ds(lo, w)], loc_sem.at[n_sem]
            )
        )
        n_sem += 1
        for cp in waits:
            cp.start()
        a_chunks.append((lo, w, waits))

    barrier = pltpu.get_barrier_semaphore()
    near = [dz for t in range(1, STRIDE + 1) for dz in (t, -t)]

    def greet(sem, dz, cores):
        for c in cores:
            pl.semaphore_signal(sem, inc=1, device_id=dev(dz, c), device_id_type=MESH)

    for dz in near:
        pl.when(relays & (z + dz < nz))(functools.partial(greet, barrier, dz, (0, 1)))
    pl.semaphore_signal(barrier, inc=1, device_id=partner, device_id_type=MESH)

    def await_near():
        pl.semaphore_wait(barrier, len(near) + 1 - jnp.maximum(STRIDE - z, 0))
        for dz in range(1, STRIDE + 1):
            pl.when(relays & (z + dz >= nz))(functools.partial(greet, wrap_sem, dz, (1,)))

    def add_product(x_ref, w_ref, lo, w, total, copies):
        for i in range(2):
            cols = slice(lo + i * (w // 2), lo + (i + 1) * (w // 2))
            p = w_ref[:, cols]
            p = jnp.concatenate([p] * copies, axis=0) if copies > 1 else p
            prod = lax.dot_general(x_ref[:, cols], p, NT, preferred_element_type=F32)
            width = prod.shape[1]
            if lo == 0:
                total[i, :, :width] = prod
            else:
                total[i, :, :width] += prod

    pout_copy.wait()
    for lo, w, cp in g_chunks:
        cp.wait()
        add_product(gbuf, poutb, lo, w, pg_sum, 1)
    pg = (pg_sum[0, :, :rank] + pg_sum[1, :, :rank]).astype(BF16)
    rows = 4 * rank
    r = lax.broadcasted_iota(jnp.int32, (rows, rank), 0)
    i = lax.broadcasted_iota(jnp.int32, (rows, rank), 1)
    quarter = r // rank
    i_lo = (quarter & 1) * 2 + quarter // 2
    spread = (i == ((r & (rank - 1)) & ~3) + i_lo).astype(F32).astype(BF16)
    wide = lax.dot_general(spread, pg, NT, preferred_element_type=F32)
    e = lax.broadcasted_iota(jnp.int32, (8, toks), 0) & 3
    tok = lax.broadcasted_iota(jnp.int32, (8, toks), 1)
    end0 = lens[0, 0]
    end1 = end0 + lens[0, 1]
    end2 = end1 + lens[0, 2]
    owner = (
        (tok >= end0).astype(jnp.int32)
        + (tok >= end1).astype(jnp.int32)
        + (tok >= end2).astype(jnp.int32)
    )
    member = (owner == e)[None]
    lhs = jnp.where(member, wide.reshape(rows // 8, 8, toks), 0.0).reshape(rows, toks).astype(BF16)

    slot = part * 2 + core
    def q_send(dz, index, to):
        return remote(qs.at[:, q_cols(dz)], qbuf.at[slot], qsend, qrecv.at[index], to)

    q_up = q_send(1, core, dev(1))
    q_down = q_send(-1, 2 + core, dev(-1))
    q_far = q_send(2, 4 + core, {"dp": lax.rem(z + nz + 2 - 4 * core, nz) * 2 + 1})
    q_near = q_send(0, 6, partner)
    for n, (lo, w, waits) in enumerate(a_chunks):
        if n == min(1, len(a_chunks) - 1):
            await_near()
            q_up.start()
            pl.when(core == 0)(q_near.start)
            pl.when((z >= STRIDE) | (core == 0))(q_far.start)
            pl.when(z >= STRIDE)(q_down.start)
        for cp in waits:
            cp.wait()
        add_product(abuf, pinb, lo, w, pa_sum, 2)
    pa = pa_sum[0] + pa_sum[1]
    left = lax.broadcasted_iota(jnp.int32, (toks, 2 * rank), 1) < rank
    pa_l = jnp.where(left, pa, 0.0).astype(BF16)
    pa_r = jnp.where(left, 0.0, pa).astype(BF16)
    half = 2 * rank
    y = jnp.dot(lhs[:half], pa_l, preferred_element_type=F32) + jnp.dot(
        lhs[half:], pa_r, preferred_element_type=F32
    )
    y = jnp.concatenate([y[:rank], y[rank:]], axis=1).astype(BF16)
    own_rows = rank // STRIDE
    for s in range(STRIDE):
        ybuf[s] = y[s * own_rows : (s + 1) * own_rows]

    groups, blocks = nz // (2 * STRIDE), 2 * STRIDE
    own = nz - 1

    def slot_of(i, up):
        return (i - 1) // STRIDE * blocks + (0 if up else STRIDE) + (i - 1) % STRIDE

    def leg(up, t):
        dz = t if up else -t
        k = 2 * slot_of(t, up) + core
        return remote(
            ybuf.at[lax.rem(z + nz + dz, STRIDE)], rbuf.at[k], dsend, erecv.at[k], dev(dz)
        )

    hops = range(STRIDE, 0, -1)
    ups = [leg(True, t) for t in hops]
    downs = [leg(False, t) for t in hops if slot_of(t, False) != own]
    for cp in ups:
        cp.start()

    def start_downs():
        for cp in downs:
            cp.start()

    def after_wrap():
        pl.semaphore_wait(wrap_sem, core * (STRIDE - z) + (1 - core))

        @pl.when(relays)
        def _():
            pl.semaphore_signal(wrap_sem, inc=1, device_id=partner, device_id_type=MESH)

        start_downs()
        q_down.start()
        pl.when(core == 1)(q_far.start)

    pl.when(z >= STRIDE)(start_downs)
    aside = remote(ybuf.at[part], rbuf.at[2 * own], dsend, erecv.at[2 * own], partner)

    def take(i, up):
        k = slot_of(i, up)
        nxt = k + blocks
        for c in (1, 0):
            here = rbuf.at[2 * k + c]
            remote(here, here, fsend, erecv.at[2 * k + c], partner).wait_recv()
            if nxt < own:
                there = 2 * nxt + c
                remote(
                    here, rbuf.at[there], fsend, erecv.at[there], dev(STRIDE if up else -STRIDE)
                ).start()

    def back(k, dz, c):
        return remote(sbuf.at[2 * k + c], res.at[z], rsend, rrecv, dev(dz, c))

    def score(step):
        count = 2 * blocks
        sub = lax.broadcasted_iota(jnp.int32, (count, 8, 128), 1) < 4
        slots = slice(step * count, (step + 1) * count)
        held = rbuf[slots].reshape(count * own_rows, 4 * rank)
        prods = []
        for i in range(STRIDE):
            w = qbuf[:, :, i * 256 : (i + 1) * 256].reshape(-1, 256)
            pr = lax.dot_general(held, w, NT, preferred_element_type=F32)
            pr = pr.reshape(count, own_rows, pr.shape[-1])
            prods.append(pr[:, 8 * (i // 2) : 8 * (i // 2) + 8])
        packed = []
        for h in range(2):
            c0, c1 = h * 128, (h + 1) * 128
            s = jnp.where(sub, prods[0][:, :, c0:c1], prods[1][:, :, c0:c1])
            s = s + jnp.where(sub, prods[2][:, :, c0:c1], prods[3][:, :, c0:c1])
            packed.append(s + pltpu.roll(s, 4, 1))
        sbuf[slots] = jnp.where(sub, packed[0], packed[1]).astype(BF16)
        for t in range(STRIDE, 0, -1):
            i = step * STRIDE + t
            for c in range(2):
                back(slot_of(i, True), -i, c).start()
                if slot_of(i, False) != own:
                    back(slot_of(i, False), i, c).start()

    def sent(ref, count, sem):
        many = ref.at[pl.ds(0, count)]
        remote(many, many, sem, rrecv, partner).wait_send()

    def returned(count):
        many = res.at[pl.ds(0, count)]
        remote(many, many, rsend, rrecv, partner).wait_recv()

    @pl.when(core == 0)
    def _():
        aside.start()
        pl.when(z < STRIDE)(after_wrap)
        sent(qbuf, 4, qsend)
        sent(rbuf, len(ups) + len(downs) + 1, dsend)
        returned(nz)

    @pl.when(core == 1)
    def _():
        rbuf[2 * own + 1] = ybuf[part]
        q_own.wait()
        for step in range(groups):
            for t in range(1, STRIDE + 1):
                if step == 0:
                    pl.when(z == t - 1)(after_wrap)
                take(step * STRIDE + t, True)
            for t in range(1, STRIDE + 1):
                if slot_of(step * STRIDE + t, False) != own:
                    take(step * STRIDE + t, False)
            if step == 0:
                for k in range(7):
                    remote(qbuf.at[k], qbuf.at[k], qsend, qrecv.at[k], partner).wait_recv()
            if step == groups - 1:
                aside.wait_recv()
            score(step)
        other = remote(sbuf.at[2 * own], res.at[z], rsend, rrecv, partner)
        other.start()
        res[z] = sbuf[2 * own + 1]
        sent(qbuf, 3, qsend)
        sent(rbuf, len(ups) + len(downs), dsend)
        if own > blocks:
            sent(rbuf, 2 * (own - blocks), fsend)
        sent(sbuf, 2 * own + 1, rsend)
        returned(own)

    quads = nz // STRIDE
    row = lax.broadcasted_iota(jnp.int32, (8, 128), 0)
    lane = lax.broadcasted_iota(jnp.int32, (8, 128), 1)
    col = (row // 4) * 128 + lane
    masks = []
    for rho in range(STRIDE):
        gap = (col // 64 - rho + STRIDE) & (STRIDE - 1)
        shift = jnp.where(gap == 3, -1, gap)
        shift = jnp.where(gap == 2, jnp.where((col // 32) % 2 == 0, -2, 2), shift)
        target = rho + shift
        masks.append((rho, 0, (target >= 0) & (target < STRIDE)))
        if rho < 2:
            masks.append((rho, -1, target < 0))
        else:
            masks.append((rho, 1, target >= STRIDE))

    def add_up(seg, carry):
        total = jnp.zeros((8, 128), F32)
        for rho, rel, mask in masks:
            val = res[lax.rem(seg + quads - rel, quads) * STRIDE + rho].astype(F32)
            total = total + jnp.where(mask, val, 0.0)
        out[seg] = total.astype(out.dtype)
        return carry

    lax.fori_loop(0, quads, add_up, 0)


def local(nz, activations, out_grads, lengths, proj_in, proj_out, queries):
    toks, ff = activations.shape
    d = out_grads.shape[1]
    rank = proj_in.shape[1]
    nq, params = queries.shape
    chunk = min(2048, d)
    n_loc = 3 + len(cuts(d, chunk)) + len(cuts(ff, chunk))
    dma = pltpu.SemaphoreType.DMA
    anyspec = pl.BlockSpec(memory_space=pl.ANY)
    rows = rank // STRIDE
    scores = pl.pallas_call(
        functools.partial(kernel, nz, chunk),
        out_shape=jax.ShapeDtypeStruct((nz // STRIDE, 8, 128), BF16),
        in_specs=[
            anyspec, anyspec, pl.BlockSpec(memory_space=pltpu.SMEM), anyspec, anyspec, anyspec,
        ],
        out_specs=pl.BlockSpec(memory_space=pltpu.VMEM),
        scratch_shapes=[
            pltpu.VMEM((toks, ff), BF16),
            pltpu.VMEM((toks, d), BF16),
            pltpu.VMEM((rank, ff), BF16),
            pltpu.VMEM((rank, d), BF16),
            pltpu.VMEM((2 * STRIDE, nq, params // STRIDE), BF16),
            pltpu.VMEM((STRIDE, rows, 4 * rank), BF16),
            pltpu.VMEM((2 * nz, rows, 4 * rank), BF16),
            pltpu.VMEM((2 * nz, 8, 128), BF16),
            pltpu.VMEM((nz, 8, 128), BF16),
            dma((n_loc,)), dma(()), dma(()), dma((7,)), dma(()),
            dma(()), dma((2 * nz,)), dma(()), dma(()), pltpu.SemaphoreType.REGULAR,
            pltpu.VMEM((2, toks, 2 * rank), F32),
            pltpu.VMEM((2, toks, 2 * rank), F32),
        ],
        compiler_params=pltpu.CompilerParams(collective_id=0, has_side_effects=True),
        name="score",
    )(activations, out_grads, lengths, proj_in.T, proj_out.T, queries)
    scores = scores.reshape(nz // STRIDE, 2, 4, 128).transpose(2, 0, 1, 3)
    return scores.reshape(lengths.shape[1], 2 * nz * nq)


def solution(mesh):
    both = P(("parts", "dp"), None)
    in_specs = (both, both, both, P(), P(), both)
    body = functools.partial(local, mesh.shape["dp"] // 2)
    return jax.shard_map(body, mesh=mesh, in_specs=in_specs, out_specs=both, check_vma=False)
```

```python
import functools

import jax
import jax.numpy as jnp
from jax import lax
from jax.experimental import pallas as pl
from jax.experimental.pallas import tpu as pltpu
from jax.sharding import PartitionSpec as P

MESH = pl.DeviceIdType.MESH
STRIDE = 4
F32 = jnp.float32
BF16 = jnp.bfloat16
NT = (((1,), (1,)), ((), ()))


def cuts(total, size):
    widths = [size] * (total // size)
    if total % size:
        widths.append(total % size)
    if widths[-1] % 256 == 0 and widths[-1] >= 512:
        widths[-1:] = [widths[-1] // 2] * 2
    starts = [sum(widths[:i]) for i in range(len(widths))]
    return list(zip(starts, widths))


def kernel(
    nz, chunk, acts, grads, lens, pin, pout, qs, out,
    abuf, gbuf, pinb, poutb, qbuf, ybuf, rbuf, sbuf, res,
    loc_sem, qloc_sem, qsend, qrecv, dsend, fsend, erecv, rsend, rrecv, wrap_sem, pg_sum, pa_sum,
):
    me = lax.axis_index("dp")
    z, core = me // 2, lax.rem(me, 2)
    part = lax.rem(z, STRIDE)
    toks, ff = acts.shape
    d = grads.shape[1]
    rank = pin.shape[0]
    kq = qs.shape[1] // STRIDE

    def chip(dz):
        return lax.rem(z + nz + dz, nz)

    def dev(dz):
        return {"dp": chip(dz) * 2 + core}

    partner = {"dp": z * 2 + 1 - core}

    def remote(src, dst, ssem, rsem, to):
        return pltpu.make_async_remote_copy(
            src_ref=src, dst_ref=dst, send_sem=ssem, recv_sem=rsem,
            device_id=to, device_id_type=MESH,
        )

    def q_cols(dz):
        return pl.ds(pl.multiple_of(lax.rem(z + nz + dz, STRIDE) * kq, kq), kq)

    n_sem = 0
    g_chunks, a_chunks = [], []
    pout_copy = pltpu.make_async_copy(pout, poutb, loc_sem.at[n_sem])
    pout_copy.start()
    n_sem += 1
    for lo, w in cuts(d, chunk):
        cp = pltpu.make_async_copy(
            grads.at[:, pl.ds(lo, w)], gbuf.at[:, pl.ds(lo, w)], loc_sem.at[n_sem]
        )
        cp.start()
        n_sem += 1
        g_chunks.append((lo, w, cp))
    q_own = pltpu.make_async_copy(qs.at[:, q_cols(0)], qbuf.at[part * 2 + core], qloc_sem)
    q_own.start()
    pieces = cuts(ff, chunk)
    middle = pieces[len(pieces) // 2][0]
    halves = {0: slice(0, middle), middle: slice(middle, ff)}
    for lo, w in pieces:
        waits = []
        if lo in halves:
            cols = halves[lo]
            waits.append(
                pltpu.make_async_copy(pin.at[:, cols], pinb.at[:, cols], loc_sem.at[n_sem])
            )
            n_sem += 1
        waits.append(
            pltpu.make_async_copy(
                acts.at[:, pl.ds(lo, w)], abuf.at[:, pl.ds(lo, w)], loc_sem.at[n_sem]
            )
        )
        n_sem += 1
        for cp in waits:
            cp.start()
        a_chunks.append((lo, w, waits))

    barrier = pltpu.get_barrier_semaphore()
    near = [dz for t in range(1, STRIDE + 1) for dz in (t, -t)]

    def greet(sem, dz):
        pl.semaphore_signal(sem, inc=1, device_id=dev(dz), device_id_type=MESH)

    for dz in near:
        if dz < 0:
            greet(barrier, dz)
        else:
            pl.when(z + dz < nz)(functools.partial(greet, barrier, dz))
    pl.semaphore_signal(barrier, inc=1, device_id=partner, device_id_type=MESH)

    def await_near():
        pl.semaphore_wait(barrier, len(near) + 1 - jnp.maximum(STRIDE - z, 0))
        for dz in range(1, STRIDE + 1):
            pl.when(z + dz >= nz)(functools.partial(greet, wrap_sem, dz))

    def add_product(x_ref, w_ref, lo, w, total, copies):
        for i in range(2):
            cols = slice(lo + i * (w // 2), lo + (i + 1) * (w // 2))
            p = w_ref[:, cols]
            p = jnp.concatenate([p] * copies, axis=0) if copies > 1 else p
            prod = lax.dot_general(x_ref[:, cols], p, NT, preferred_element_type=F32)
            width = prod.shape[1]
            if lo == 0:
                total[i, :, :width] = prod
            else:
                total[i, :, :width] += prod

    pout_copy.wait()
    for lo, w, cp in g_chunks:
        cp.wait()
        add_product(gbuf, poutb, lo, w, pg_sum, 1)
    pg = (pg_sum[0, :, :rank] + pg_sum[1, :, :rank]).astype(BF16)
    rows = 4 * rank
    r = lax.broadcasted_iota(jnp.int32, (rows, rank), 0)
    i = lax.broadcasted_iota(jnp.int32, (rows, rank), 1)
    quarter = r // rank
    i_lo = (quarter & 1) * 2 + quarter // 2
    spread = (i == ((r & (rank - 1)) & ~3) + i_lo).astype(F32).astype(BF16)
    wide = lax.dot_general(spread, pg, NT, preferred_element_type=F32)
    e = lax.broadcasted_iota(jnp.int32, (8, toks), 0) & 3
    tok = lax.broadcasted_iota(jnp.int32, (8, toks), 1)
    end0 = lens[0, 0]
    end1 = end0 + lens[0, 1]
    end2 = end1 + lens[0, 2]
    owner = (
        (tok >= end0).astype(jnp.int32)
        + (tok >= end1).astype(jnp.int32)
        + (tok >= end2).astype(jnp.int32)
    )
    member = (owner == e)[None]
    lhs = jnp.where(member, wide.reshape(rows // 8, 8, toks), 0.0).reshape(rows, toks).astype(BF16)

    slot = part * 2 + core
    q_up = remote(qs.at[:, q_cols(1)], qbuf.at[slot], qsend, qrecv.at[0], dev(1))
    q_down = remote(qs.at[:, q_cols(-1)], qbuf.at[slot], qsend, qrecv.at[1], dev(-1))
    far = {"dp": lax.rem(z + nz + 2 - 4 * core, nz) * 2 + core}
    q_far = remote(qs.at[:, q_cols(2)], qbuf.at[slot], qsend, qrecv.at[2], far)
    q_near = remote(qs.at[:, q_cols(0)], qbuf.at[slot], qsend, qrecv.at[3], partner)
    q_sends = [q_up, q_down, q_far, q_near]
    for n, (lo, w, waits) in enumerate(a_chunks):
        if n == min(1, len(a_chunks) - 1):
            await_near()
            q_up.start()
            q_near.start()
            pl.when((z >= STRIDE) | (core == 0))(q_far.start)
            pl.when(z >= STRIDE)(q_down.start)
        for cp in waits:
            cp.wait()
        add_product(abuf, pinb, lo, w, pa_sum, 2)
    pa = pa_sum[0] + pa_sum[1]
    left = lax.broadcasted_iota(jnp.int32, (toks, 2 * rank), 1) < rank
    pa_l = jnp.where(left, pa, 0.0).astype(BF16)
    pa_r = jnp.where(left, 0.0, pa).astype(BF16)
    half = 2 * rank
    y = jnp.dot(lhs[:half], pa_l, preferred_element_type=F32) + jnp.dot(
        lhs[half:], pa_r, preferred_element_type=F32
    )
    y = jnp.concatenate([y[:rank], y[rank:]], axis=1).astype(BF16)
    own_rows = rank // STRIDE
    for s in range(STRIDE):
        ybuf[s] = y[s * own_rows : (s + 1) * own_rows]

    groups, blocks = nz // (2 * STRIDE), 2 * STRIDE
    own = nz - 1

    def slot_of(i, up):
        return (i - 1) // STRIDE * blocks + (0 if up else STRIDE) + (i - 1) % STRIDE

    def leg(up, t):
        dz = t if up else -t
        k = slot_of(t, up)
        return remote(
            ybuf.at[lax.rem(z + nz + dz, STRIDE)], rbuf.at[k], dsend, erecv.at[k], dev(dz)
        )

    hops = range(STRIDE, 0, -1)
    ups = [leg(True, t) for t in hops]
    downs = [leg(False, t) for t in hops if slot_of(t, False) != own]
    for cp in ups:
        cp.start()

    def start_downs():
        for cp in downs:
            cp.start()

    def after_wrap():
        pl.semaphore_wait(wrap_sem, STRIDE - z)
        start_downs()
        q_down.start()
        pl.when(core == 1)(q_far.start)

    pl.when(z >= STRIDE)(start_downs)
    rbuf[own] = ybuf[part]
    q_own.wait()

    def take(i, up):
        k = slot_of(i, up)
        remote(rbuf.at[k], rbuf.at[k], fsend, erecv.at[k], partner).wait_recv()
        nxt = k + blocks
        if nxt < own:
            remote(
                rbuf.at[k], rbuf.at[nxt], fsend, erecv.at[nxt],
                dev(STRIDE if up else -STRIDE),
            ).start()

    sub = lax.broadcasted_iota(jnp.int32, (blocks, 8, 128), 1) < 4

    def back(k, dz):
        return remote(sbuf.at[k], res.at[z], rsend, rrecv, dev(dz))

    def score(step):
        slots = slice(step * blocks, (step + 1) * blocks)
        held = rbuf[slots].reshape(blocks * own_rows, 4 * rank)
        prods = []
        for i in range(STRIDE):
            w = qbuf[:, :, i * 256 : (i + 1) * 256].reshape(-1, 256)
            pr = lax.dot_general(held, w, NT, preferred_element_type=F32)
            pr = pr.reshape(blocks, own_rows, pr.shape[-1])
            prods.append(pr[:, 8 * (i // 2) : 8 * (i // 2) + 8])
        packed = []
        for h in range(2):
            c0, c1 = h * 128, (h + 1) * 128
            s = jnp.where(sub, prods[0][:, :, c0:c1], prods[1][:, :, c0:c1])
            s = s + jnp.where(sub, prods[2][:, :, c0:c1], prods[3][:, :, c0:c1])
            packed.append(s + pltpu.roll(s, 4, 1))
        sbuf[slots] = jnp.where(sub, packed[0], packed[1]).astype(BF16)
        for t in range(STRIDE, 0, -1):
            i = step * STRIDE + t
            back(slot_of(i, True), -i).start()
            if slot_of(i, False) != own:
                back(slot_of(i, False), i).start()

    passed = []
    for step in range(groups):
        def take_ups(step=step):
            for t in range(1, STRIDE + 1):
                take(step * STRIDE + t, True)

        def take_downs(step=step):
            for t in range(1, STRIDE + 1):
                if slot_of(step * STRIDE + t, False) != own:
                    take(step * STRIDE + t, False)

        down_first = (z < nz // 2) & (z < (step + 1) * STRIDE)

        def down_then_up(step=step):
            if step == 0:
                after_wrap()
            take_downs(step)
            take_ups(step)

        def up_then_down(step=step):
            take_ups(step)
            take_downs(step)

        if step < 2:
            pl.when(down_first)(down_then_up)
            pl.when(jnp.logical_not(down_first))(up_then_down)
        else:
            up_then_down(step)
        if step == 0:
            for k, dz in enumerate((-1, 1, 2)):
                came = lax.rem(z + nz + dz, STRIDE) * 2 + core
                q_sends[k].wait_recv()
                passed.append(
                    remote(
                        qbuf.at[came], qbuf.at[came], qsend, qrecv.at[4 + k], partner
                    )
                )
                passed[-1].start()
        if step == 0:
            q_near.wait_recv()
            for cp in passed:
                cp.wait_recv()
        score(step)
    res[z] = sbuf[own]

    def sent(ref, count, sem):
        many = ref.at[pl.ds(0, count)]
        remote(many, many, sem, rrecv, partner).wait_send()

    sent(qbuf, len(q_sends) + len(passed), qsend)
    sent(rbuf, len(ups) + len(downs), dsend)
    if own > blocks:
        sent(rbuf, own - blocks, fsend)
    sent(sbuf, own, rsend)
    others = res.at[pl.ds(0, own)]
    remote(others, others, rsend, rrecv, partner).wait_recv()

    quads = nz // STRIDE
    row = lax.broadcasted_iota(jnp.int32, (8, 128), 0)
    lane = lax.broadcasted_iota(jnp.int32, (8, 128), 1)
    col = (row // 4) * 128 + lane
    masks = []
    for rho in range(STRIDE):
        gap = (col // 64 - rho + STRIDE) & (STRIDE - 1)
        shift = jnp.where(gap == 3, -1, gap)
        shift = jnp.where(gap == 2, jnp.where((col // 32) % 2 == 0, -2, 2), shift)
        target = rho + shift
        masks.append((rho, 0, (target >= 0) & (target < STRIDE)))
        if rho < 2:
            masks.append((rho, -1, target < 0))
        else:
            masks.append((rho, 1, target >= STRIDE))

    def add_up(seg, carry):
        total = jnp.zeros((8, 128), F32)
        for rho, rel, mask in masks:
            val = res[lax.rem(seg + quads - rel, quads) * STRIDE + rho].astype(F32)
            total = total + jnp.where(mask, val, 0.0)
        out[seg] = total.astype(out.dtype)
        return carry

    lax.fori_loop(0, quads, add_up, 0)


def local(nz, activations, out_grads, lengths, proj_in, proj_out, queries):
    toks, ff = activations.shape
    d = out_grads.shape[1]
    rank = proj_in.shape[1]
    nq, params = queries.shape
    chunk = min(2048, d)
    n_loc = 3 + len(cuts(d, chunk)) + len(cuts(ff, chunk))
    dma = pltpu.SemaphoreType.DMA
    anyspec = pl.BlockSpec(memory_space=pl.ANY)
    rows = rank // STRIDE
    scores = pl.pallas_call(
        functools.partial(kernel, nz, chunk),
        out_shape=jax.ShapeDtypeStruct((nz // STRIDE, 8, 128), BF16),
        in_specs=[
            anyspec, anyspec, pl.BlockSpec(memory_space=pltpu.SMEM), anyspec, anyspec, anyspec,
        ],
        out_specs=pl.BlockSpec(memory_space=pltpu.VMEM),
        scratch_shapes=[
            pltpu.VMEM((toks, ff), BF16),
            pltpu.VMEM((toks, d), BF16),
            pltpu.VMEM((rank, ff), BF16),
            pltpu.VMEM((rank, d), BF16),
            pltpu.VMEM((2 * STRIDE, nq, params // STRIDE), BF16),
            pltpu.VMEM((STRIDE, rows, 4 * rank), BF16),
            pltpu.VMEM((nz, rows, 4 * rank), BF16),
            pltpu.VMEM((nz, 8, 128), BF16),
            pltpu.VMEM((nz, 8, 128), BF16),
            dma((n_loc,)), dma(()), dma(()), dma((7,)), dma(()),
            dma(()), dma((nz,)), dma(()), dma(()), pltpu.SemaphoreType.REGULAR,
            pltpu.VMEM((2, toks, 2 * rank), F32),
            pltpu.VMEM((2, toks, 2 * rank), F32),
        ],
        compiler_params=pltpu.CompilerParams(collective_id=0, has_side_effects=True),
        name="score",
    )(activations, out_grads, lengths, proj_in.T, proj_out.T, queries)
    scores = scores.reshape(nz // STRIDE, 2, 4, 128).transpose(2, 0, 1, 3)
    return scores.reshape(lengths.shape[1], 2 * nz * nq)


def solution(mesh):
    both = P(("parts", "dp"), None)
    in_specs = (both, both, both, P(), P(), both)
    body = functools.partial(local, mesh.shape["dp"] // 2)
    return jax.shard_map(body, mesh=mesh, in_specs=in_specs, out_specs=both, check_vma=False)
```
